64 devices in a mesh: kv: 4 (over x, y), dup: 16 (over z, core).
Axes of the slice: x: 2, y: 2, z: 8, core: 2. Of those that a mesh axis runs over, the one named last changes fastest.
The devices are a block of a 4x4x8 slice.
Arguments:
- queries: bfloat16 [1024, 64, 128], P('kv', 'dup'), parts along dimension 0
- key_cache: bfloat16 [1024, 2048, 128], P('kv', 'dup'), parts along dimension 0
- value_cache: bfloat16 [1024, 2048, 128], P('kv', 'dup'), parts along dimension 0
- lengths: int32 [1024], P('kv'), parts along dimension 0
Outputs:
- output: bfloat16 [1024, 64, 128], P('kv', 'dup'), parts along dimension 0
There are 4 independent parts. The reference program is written for one: setup_inputs(seed, part) draws one part's arguments, and reference() takes and returns one part's arrays. A program takes and returns all parts, laid end to end along the dimension named above; each array names one.
All inputs are finite; a program needn't handle non-finite values.
Results may differ from the reference program's by a relative error of at most 0.00814941.
Values are sent between devices in bfloat16 or wider.
A program may use at most 768 MiB of HBM per device.

```python
import math
import jax
import jax.numpy as jnp
from jax import lax

BATCH = 256
SEQ = 2048
HEADS = 32
KV_HEADS = 2
HEAD_DIM = 128
DRAFT = 4

GROUP_HEADS = HEADS // KV_HEADS
QUERY_ROWS = GROUP_HEADS * DRAFT


def wave_field(k_freq, k_phase, k_dir, strength):
    spot_frac = jnp.arange(SEQ, dtype=jnp.float32) / SEQ
    freq_row = jax.random.randint(k_freq, (BATCH, 3), 1, 17, jnp.int32).astype(jnp.float32)
    phases = jax.random.uniform(k_phase, (BATCH, 3), jnp.float32) * (2.0 * math.pi)
    directions = jax.random.normal(k_dir, (BATCH, 3, HEAD_DIM), jnp.float32)
    wave_vals = jnp.cos(2.0 * math.pi * freq_row[:, None, :] * spot_frac[None, :, None] + phases[:, None, :])
    return strength * jnp.einsum("bsk,bkd->bsd", wave_vals, directions)


def setup_inputs(seed: int = 0, part: int = 0) -> dict:
    part_key = jax.random.fold_in(jax.random.key(seed), part)
    key_list = jax.random.split(part_key, 11)
    queries = jax.random.normal(key_list[0], (BATCH, QUERY_ROWS, HEAD_DIM), jnp.float32)
    k_noise = jax.random.normal(key_list[1], (BATCH, SEQ, HEAD_DIM), jnp.float32)
    key_cache = k_noise + wave_field(key_list[2], key_list[3], key_list[4], 1.5)
    v_noise = jax.random.normal(key_list[5], (BATCH, SEQ, HEAD_DIM), jnp.float32)
    value_cache = v_noise + wave_field(key_list[6], key_list[7], key_list[8], 1.0)
    low_len = max(DRAFT, SEQ // 8)
    lengths = jax.random.randint(key_list[9], (BATCH,), low_len, SEQ + 1, jnp.int32)
    full_row = jax.random.randint(key_list[10], (), 0, BATCH, jnp.int32)
    lengths = jnp.where(jnp.arange(BATCH) == full_row, SEQ, lengths).astype(jnp.int32)
    return {"queries": queries.astype(jnp.bfloat16), "key_cache": key_cache.astype(jnp.bfloat16), "value_cache": value_cache.astype(jnp.bfloat16), "lengths": lengths}


def reference(queries, key_cache, value_cache, lengths):
    score_scale = 1.0 / math.sqrt(HEAD_DIM)
    draft_pos = jnp.arange(QUERY_ROWS) % DRAFT
    seq_pos = jnp.arange(SEQ)

    def one_sequence(operands):
        q_rows, k_rows, v_rows, length = operands
        scores = jnp.dot(q_rows, k_rows.T, preferred_element_type=jnp.float32) * score_scale
        last_pos = length - DRAFT + draft_pos
        allowed = seq_pos[None, :] <= last_pos[:, None]
        scores = jnp.where(allowed, scores, -jnp.inf)
        row_peak = jnp.max(scores, axis=1, keepdims=True)
        prob_vals = jnp.exp(scores - row_peak)
        row_mass = jnp.sum(prob_vals, axis=1, keepdims=True)
        weighted = jnp.dot(prob_vals.astype(jnp.bfloat16), v_rows, preferred_element_type=jnp.float32)
        return (weighted / row_mass).astype(jnp.bfloat16)

    return lax.map(one_sequence, (queries, key_cache, value_cache, lengths))
```

```python
import functools
import math

import jax
import jax.numpy as jnp
from jax import lax
from jax.experimental import pallas as pl
from jax.experimental.pallas import tpu as pltpu
from jax.sharding import PartitionSpec as P

DRAFT = 4
NEG_BIG = -1e30
LANES = 128
GROUP = 16
MESH_ID = pl.DeviceIdType.MESH

SKEW_GATHER = (0, 1, 2, 3, 4)
SKEW_COMPUTE = 5
SKEW_REDUCE = (10, 9, 8, 7, 6)


def kernel(ring, len_ref, q_hbm, k_hbm, v_hbm, out_hbm,
           q_all, o_all, o_pair, o_in, o_half, s_all, s_pair, s_in, k_buf, v_buf, out_buf, s_acc,
           q_sem, k_sem, v_sem, out_sem, ag_send, ag_recv, pq_send, pq_recv,
           po_send, po_recv, ps_send, ps_recv, rs_send, rs_recv, ss_send, ss_recv):
    half = ring // 2
    num_chunks = s_all.shape[1]
    rows = LANES
    half_rows = rows // 2
    seqs = rows // DRAFT
    head_dim = q_hbm.shape[-1]
    span_len = k_hbm.shape[1]

    me = lax.axis_index("dup")
    z = me // 2
    core = lax.rem(me, 2)
    partner = me + 1 - 2 * core
    right = lax.rem(z + 1, ring) * 2 + core
    left = lax.rem(z + ring - 1, ring) * 2 + core
    beside = (right, left)

    def load_kv(c):
        span = pl.ds(c * seqs, seqs)
        return (pltpu.make_async_copy(k_hbm.at[span], k_buf.at[span], k_sem.at[c]),
                pltpu.make_async_copy(v_hbm.at[span], v_buf.at[span], v_sem.at[c]))

    load_q = pltpu.make_async_copy(q_hbm, q_all.at[0, 0], q_sem)
    load_q.start()

    barrier = pltpu.get_barrier_semaphore()
    for other in (right, left, partner):
        pl.semaphore_signal(barrier, inc=1, device_id={"dup": other}, device_id_type=MESH_ID)

    @pl.loop(0, num_chunks)
    def _(c):
        for copy in load_kv(c):
            copy.start()

    load_q.wait()
    pl.semaphore_wait(barrier, 3)

    def send(src, dst, send_sem, recv_sem, other):
        return pltpu.make_async_remote_copy(src_ref=src, dst_ref=dst, send_sem=send_sem, recv_sem=recv_sem,
                                            device_id={"dup": other}, device_id_type=MESH_ID)

    def arrived(ref, sem):
        pltpu.make_async_copy(ref, ref, sem).wait()

    def chunk_rows(c):
        return pl.ds(pl.multiple_of(c * rows, rows), rows)

    def split_rows(c, way):
        return pl.ds(pl.multiple_of(c * rows + way * half_rows, half_rows), half_rows)

    def half_rows_of(c):
        return pl.ds(pl.multiple_of(c * half_rows, half_rows), half_rows)

    def slot_at(way, hop):
        return lax.rem(ring - hop, ring) if way == 0 else hop

    def gather(hop, c):
        area = chunk_rows(c)
        slots = [(ring - hop) % ring, hop % ring]
        if 0 < hop < half:
            for way in range(2):
                arrived(q_all.at[0, slots[way], area], ag_recv.at[c, way, hop - 1])
        elif hop == half:
            for way in range(2):
                arrived(q_all.at[0, half, split_rows(c, way)], ag_recv.at[c, way, hop - 1])
        if hop < half:
            for way in range(2):
                part = area if hop + 1 < half else split_rows(c, way)
                to = (ring - hop - 1) if way == 0 else hop + 1
                send(q_all.at[0, slots[way], part], q_all.at[0, to, part],
                     ag_send.at[way, hop], ag_recv.at[c, way, hop], beside[way]).start()
        for slot in sorted(set(slots)):
            send(q_all.at[0, slot, area], q_all.at[1, slot, area], pq_send, pq_recv.at[c], partner).start()

    sub = lax.broadcasted_iota(jnp.int32, (8, LANES), 0)
    lane = lax.broadcasted_iota(jnp.int32, (8, LANES), 1)
    low = (sub < DRAFT)[None]
    lane_less_token = lane - lax.rem(sub, DRAFT)
    scale = math.log2(math.e) / math.sqrt(head_dim)

    def compute(c):
        area = chunk_rows(c)
        arrived(q_all.at[1, :, area], pq_recv.at[c])
        for copy in load_kv(c):
            copy.wait()
        s_acc[...] = jnp.zeros_like(s_acc)

        @pl.loop(0, seqs // GROUP)
        def _(g):
            first = g * GROUP
            r0 = pl.multiple_of(c * rows + first * DRAFT, GROUP * DRAFT)
            q = q_all[:, :, pl.ds(r0, GROUP * DRAFT), :].astype(jnp.float32)
            q = q.reshape(2, ring, GROUP // 2, 8, head_dim)
            acc = s_acc[...]
            outs = []
            for pair in range(GROUP // 2):
                mine, theirs = q[0, :, pair], q[1, :, pair]
                both = (jnp.where(low, mine, pltpu.roll(theirs, DRAFT, 1)), jnp.where(low, pltpu.roll(mine, DRAFT, 1), theirs))
                pair_out = []
                for odd in range(2):
                    local = first + 2 * pair + odd
                    seq = c * seqs + local
                    q_rows = both[odd].reshape(ring * 8, head_dim).astype(jnp.bfloat16)
                    s = lax.dot_general(q_rows, k_buf[seq], (((1,), (1,)), ((), ())), preferred_element_type=jnp.float32)
                    limit = len_ref[seq] - DRAFT - me * span_len
                    s = jnp.where((lane_less_token <= limit)[None], s.reshape(ring, 8, span_len), NEG_BIG)
                    peak = jnp.max(s, axis=2, keepdims=True)
                    p = jnp.exp2((s - peak) * scale)
                    mass = jnp.sum(p, axis=2, keepdims=True)
                    o = jnp.dot(p.astype(jnp.bfloat16).reshape(ring * 8, span_len), v_buf[seq], preferred_element_type=jnp.float32)
                    pair_out.append(o.reshape(ring, 8, head_dim) * (1.0 / mass))
                    log_mass = peak * scale + jnp.log2(mass)
                    acc = jnp.where((lane_less_token == DRAFT * local)[None], log_mass, acc)
                even, odd_ = pair_out
                outs.append((jnp.where(low, even, pltpu.roll(odd_, DRAFT, 1)), jnp.where(low, pltpu.roll(even, DRAFT, 1), odd_)))
                if pair % 2 == 1:
                    at = pl.ds(pl.multiple_of(r0 + (pair - 1) * 8, 16), 16)
                    for side in range(2):
                        tile = jnp.concatenate([outs[-2][side], outs[-1][side]], axis=1)
                        o_all[side, :, at, :] = tile.astype(jnp.bfloat16)
            s_acc[...] = acc

        acc = s_acc[...]
        mine = jnp.sum(jnp.where(low, acc, 0.0), axis=1)
        theirs = jnp.sum(jnp.where(low, 0.0, acc), axis=1)
        for slot in range(ring):
            s_all[0, c, slot] = mine[slot:slot + 1]
            s_all[1, c, slot] = theirs[slot:slot + 1]
        send(o_all.at[1, :, area], o_pair.at[:, area], po_send, po_recv.at[c], partner).start()
        send(s_all.at[1, c], s_pair.at[c], ps_send, ps_recv.at[c], partner).start()

    def weigh(stats):
        top = functools.reduce(jnp.maximum, stats)
        parts = [jnp.exp2(s - top) for s in stats]
        total = functools.reduce(jnp.add, parts)
        inv = 1.0 / total
        cols = [jnp.broadcast_to(p * inv, (LANES, LANES)).T for p in parts]
        return cols, top + jnp.log2(total)

    def mix(cols, blocks):
        return functools.reduce(jnp.add, [w * b.astype(jnp.float32) for w, b in zip(cols, blocks)])

    row_lane = lax.broadcasted_iota(jnp.int32, (1, LANES), 1)

    def reduce_hop(dist, c):
        area = chunk_rows(c)
        if dist == half:
            arrived(o_pair.at[:, area], po_recv.at[c])
            arrived(s_pair.at[c], ps_recv.at[c])
            cols, stat = weigh([s_all[0, c, half], s_pair[c, half]])
            o_all[0, half, area, :] = mix(cols, [o_all[0, half, area, :], o_pair[half, area, :]]).astype(jnp.bfloat16)
            s_all[0, c, half] = stat
            for way in range(2):
                send(o_all.at[0, half, split_rows(c, way)], o_half.at[way, half_rows_of(c)],
                     rs_send.at[way, half - 1], rs_recv.at[c, way, half - 1], beside[way]).start()
                send(s_all.at[0, c, half], s_in.at[way, half - 1, c],
                     ss_send.at[way, half - 1], ss_recv.at[c, way, half - 1], beside[way]).start()
            return
        for way in range(2):
            if dist == half - 1:
                arrived(o_half.at[way, half_rows_of(c)], rs_recv.at[c, way, dist])
            else:
                arrived(o_in.at[way, dist, area], rs_recv.at[c, way, dist])
            arrived(s_in.at[way, dist, c], ss_recv.at[c, way, dist])
            if dist == 0:
                continue
            slot = dist if way == 0 else ring - dist
            coming = s_in[way, dist, c]
            if dist == half - 1:
                coming = jnp.where((row_lane < half_rows) if way == 0 else (row_lane >= half_rows), coming, NEG_BIG)
            cols, stat = weigh([s_all[0, c, slot], s_pair[c, slot], coming])
            if dist == half - 1:
                for part in range(2):
                    at = split_rows(c, part)
                    blocks = [o_all[0, slot, at, :], o_pair[slot, at, :]]
                    if part == way:
                        blocks.append(o_half[way, half_rows_of(c), :])
                    cut = [w[part * half_rows:(part + 1) * half_rows] for w in cols]
                    o_all[0, slot, at, :] = mix(cut, blocks).astype(jnp.bfloat16)
            else:
                blocks = [o_all[0, slot, area, :], o_pair[slot, area, :], o_in[way, dist, area, :]]
                o_all[0, slot, area, :] = mix(cols, blocks).astype(jnp.bfloat16)
            s_all[0, c, slot] = stat
            send(o_all.at[0, slot, area], o_in.at[way, dist - 1, area],
                 rs_send.at[way, dist - 1], rs_recv.at[c, way, dist - 1], beside[way]).start()
            send(s_all.at[0, c, slot], s_in.at[way, dist - 1, c],
                 ss_send.at[way, dist - 1], ss_recv.at[c, way, dist - 1], beside[way]).start()
        if dist == 0:
            cols, _ = weigh([s_all[0, c, 0], s_pair[c, 0], s_in[0, 0, c], s_in[1, 0, c]])
            blocks = [o_all[0, 0, area, :], o_pair[0, area, :], o_in[0, 0, area, :], o_in[1, 0, area, :]]
            out_buf[area, :] = mix(cols, blocks).astype(jnp.bfloat16)
            pltpu.make_async_copy(out_buf.at[area], out_hbm.at[area], out_sem).start()

    stages = [(SKEW_GATHER[hop], functools.partial(gather, hop)) for hop in reversed(range(half + 1))]
    stages += [(SKEW_COMPUTE, compute)]
    stages += [(SKEW_REDUCE[dist], functools.partial(reduce_hop, dist)) for dist in range(half + 1)]

    @pl.loop(0, num_chunks + max(skew for skew, _ in stages))
    def _(step):
        for skew, stage in stages:
            c = step - skew

            @pl.when(jnp.logical_and(c >= 0, c < num_chunks))
            def _(stage=stage, c=c):
                stage(c)

    for way in range(2):
        for hop in range(half):
            area = pl.ds(0, num_chunks * (rows if hop + 1 < half else half_rows))
            arrived(q_all.at[0, hop, area], ag_send.at[way, hop])
            arrived(o_all.at[0, hop, area], rs_send.at[way, hop])
            arrived(s_in.at[way, hop], ss_send.at[way, hop])
    arrived(q_all.at[1], pq_send)
    arrived(o_all.at[1], po_send)
    arrived(s_all.at[1], ps_send)
    arrived(out_buf, out_sem)


def solution(mesh):
    dup_size = mesh.shape["dup"]
    ring = dup_size // 2
    half = ring // 2

    def group_step(q_local, k_span, v_span, len_local):
        num_batch, draft, head_dim = q_local.shape
        total_rows = num_batch * draft
        chunks = total_rows // LANES
        bf16, f32 = jnp.bfloat16, jnp.float32
        dma = pltpu.SemaphoreType.DMA
        out = pl.pallas_call(
            functools.partial(kernel, ring),
            out_shape=jax.ShapeDtypeStruct((total_rows, head_dim), bf16),
            in_specs=[pl.BlockSpec(memory_space=pltpu.SMEM)] + [pl.BlockSpec(memory_space=pl.ANY)] * 3,
            out_specs=pl.BlockSpec(memory_space=pl.ANY),
            scratch_shapes=[
                pltpu.VMEM((2, ring, total_rows, head_dim), bf16),
                pltpu.VMEM((2, ring, total_rows, head_dim), bf16),
                pltpu.VMEM((ring, total_rows, head_dim), bf16),
                pltpu.VMEM((2, half - 1, total_rows, head_dim), bf16),
                pltpu.VMEM((2, total_rows // 2, head_dim), bf16),
                pltpu.VMEM((2, chunks, ring, 1, LANES), f32),
                pltpu.VMEM((chunks, ring, 1, LANES), f32),
                pltpu.VMEM((2, half, chunks, 1, LANES), f32),
                pltpu.VMEM(k_span.shape, bf16),
                pltpu.VMEM(v_span.shape, bf16),
                pltpu.VMEM((total_rows, head_dim), bf16),
                pltpu.VMEM((ring, 8, LANES), f32),
                dma, dma((chunks,)), dma((chunks,)), dma,
                dma((2, half)), dma((chunks, 2, half)), dma, dma((chunks,)),
                dma, dma((chunks,)), dma, dma((chunks,)),
                dma((2, half)), dma((chunks, 2, half)), dma((2, half)), dma((chunks, 2, half)),
            ],
            compiler_params=pltpu.CompilerParams(collective_id=0, has_side_effects=True, vmem_limit_bytes=60 * 1024 * 1024),
        )(len_local, q_local.reshape(total_rows, head_dim), k_span, v_span)
        return out.reshape(num_batch, draft, head_dim)

    return jax.shard_map(group_step, mesh=mesh, in_specs=(P("kv", "dup", None), P("kv", "dup", None), P("kv", "dup", None), P("kv")), out_specs=P("kv", "dup", None), check_vma=False)
```

```python
import functools
import math

import jax
import jax.numpy as jnp
from jax import lax
from jax.experimental import pallas as pl
from jax.experimental.pallas import tpu as pltpu
from jax.sharding import PartitionSpec as P

DRAFT = 4
NEG_BIG = -1e30
LANES = 128
QUAD = 4
LAG = 1
MESH_ID = pl.DeviceIdType.MESH

SKEW_GATHER = (0, 2, 4, 6, 8)
SKEW_COMPUTE = 9
SKEW_REDUCE = (18, 16, 14, 12, 10)


def kernel(ring, len_ref, q_hbm, k_hbm, v_hbm, out_hbm,
           q_all, o_all, o_pair, o_in, o_half, s_all, s_pair, s_in, k_buf, v_buf, out_buf,
           q_sem, k_sem, v_sem, out_sem, ag_send, ag_recv, pq_send, pq_recv,
           po_send, po_recv, ps_send, ps_recv, rs_send, rs_recv, ss_send, ss_recv):
    half = ring // 2
    num_chunks = s_all.shape[1]
    rows = LANES
    half_rows = rows // 2
    seqs = rows // DRAFT
    head_dim = q_hbm.shape[-1]
    span_len = k_hbm.shape[1]

    me = lax.axis_index("dup")
    z = me // 2
    core = lax.rem(me, 2)
    partner = me + 1 - 2 * core
    right = lax.rem(z + 1, ring) * 2 + core
    left = lax.rem(z + ring - 1, ring) * 2 + core
    beside = (right, left)

    def load_kv(c):
        span = pl.ds(c * seqs, seqs)
        return (pltpu.make_async_copy(k_hbm.at[span], k_buf.at[span], k_sem.at[c]),
                pltpu.make_async_copy(v_hbm.at[span], v_buf.at[span], v_sem.at[c]))

    load_q = pltpu.make_async_copy(q_hbm, q_all.at[0, 0], q_sem)
    load_q.start()

    barrier = pltpu.get_barrier_semaphore()
    for other in (right, left, partner):
        pl.semaphore_signal(barrier, inc=1, device_id={"dup": other}, device_id_type=MESH_ID)

    @pl.loop(0, num_chunks)
    def _(c):
        for copy in load_kv(c):
            copy.start()

    load_q.wait()
    pl.semaphore_wait(barrier, 3)

    def send(src, dst, send_sem, recv_sem, other):
        return pltpu.make_async_remote_copy(src_ref=src, dst_ref=dst, send_sem=send_sem, recv_sem=recv_sem,
                                            device_id={"dup": other}, device_id_type=MESH_ID)

    def arrived(ref, sem):
        pltpu.make_async_copy(ref, ref, sem).wait()

    def chunk_rows(c):
        return pl.ds(pl.multiple_of(c * rows, rows), rows)

    def split_rows(c, way):
        return pl.ds(pl.multiple_of(c * rows + way * half_rows, half_rows), half_rows)

    def half_rows_of(c):
        return pl.ds(pl.multiple_of(c * half_rows, half_rows), half_rows)

    def slot_at(way, hop):
        return lax.rem(ring - hop, ring) if way == 0 else hop

    def gather(hop, c):
        area = chunk_rows(c)
        slots = [(ring - hop) % ring, hop % ring]
        if 0 < hop < half:
            for way in range(2):
                arrived(q_all.at[0, slots[way], area], ag_recv.at[c, way, hop - 1])
        elif hop == half:
            for way in range(2):
                arrived(q_all.at[0, half, split_rows(c, way)], ag_recv.at[c, way, hop - 1])
        if hop < half:
            for way in range(2):
                part = area if hop + 1 < half else split_rows(c, way)
                to = (ring - hop - 1) if way == 0 else hop + 1
                send(q_all.at[0, slots[way], part], q_all.at[0, to, part],
                     ag_send.at[way, hop], ag_recv.at[c, way, hop], beside[way]).start()
        for slot in sorted(set(slots)):
            send(q_all.at[0, slot, area], q_all.at[1, slot, area], pq_send, pq_recv.at[c], partner).start()

    sub = lax.broadcasted_iota(jnp.int32, (8, LANES), 0)
    lane = lax.broadcasted_iota(jnp.int32, (8, LANES), 1)
    low = (sub < DRAFT)[None]
    lane_less_token = lane - lax.rem(sub, DRAFT)
    scale = math.log2(math.e) / math.sqrt(head_dim)

    def compute(c):
        area = chunk_rows(c)
        arrived(q_all.at[1, :, area], pq_recv.at[c])
        for copy in load_kv(c):
            copy.wait()
        acc = jnp.zeros((ring, 8, LANES), jnp.float32)
        quads = seqs // QUAD
        scores, probs = {}, {}
        for step in range(quads + 2 * LAG):
            if step < quads:
                r0 = pl.multiple_of(c * rows + step * QUAD * DRAFT, QUAD * DRAFT)
                q = q_all[:, :, pl.ds(r0, QUAD * DRAFT), :].astype(jnp.float32).reshape(2, ring, QUAD // 2, 8, head_dim)
                for pair in range(QUAD // 2):
                    mine, theirs = q[0, :, pair], q[1, :, pair]
                    both = (jnp.where(low, mine, pltpu.roll(theirs, DRAFT, 1)), jnp.where(low, pltpu.roll(mine, DRAFT, 1), theirs))
                    for odd in range(2):
                        local = step * QUAD + 2 * pair + odd
                        q_rows = both[odd].reshape(ring * 8, head_dim).astype(jnp.bfloat16)
                        scores[local] = lax.dot_general(q_rows, k_buf[c * seqs + local], (((1,), (1,)), ((), ())),
                                                        preferred_element_type=jnp.float32)
            if 0 <= step - LAG < quads:
                for local in range((step - LAG) * QUAD, (step - LAG + 1) * QUAD):
                    limit = len_ref[c * seqs + local] - DRAFT - me * span_len
                    s = scores.pop(local).reshape(ring, 8, span_len)
                    s = jnp.where((lane_less_token <= limit)[None], s, NEG_BIG)
                    peak = jnp.max(s, axis=2, keepdims=True)
                    p = jnp.exp2((s - peak) * scale)
                    mass = jnp.sum(p, axis=2, keepdims=True)
                    acc = jnp.where((lane_less_token == DRAFT * local)[None], peak * scale + jnp.log2(mass), acc)
                    probs[local] = (p.astype(jnp.bfloat16).reshape(ring * 8, span_len), 1.0 / mass)
            if 0 <= step - 2 * LAG < quads:
                outs = []
                for local in range((step - 2 * LAG) * QUAD, (step - 2 * LAG + 1) * QUAD):
                    p, inv = probs.pop(local)
                    o = jnp.dot(p, v_buf[c * seqs + local], preferred_element_type=jnp.float32)
                    outs.append(o.reshape(ring, 8, head_dim) * inv)
                sides = [[], []]
                for even, odd_ in zip(outs[0::2], outs[1::2]):
                    sides[0].append(jnp.where(low, even, pltpu.roll(odd_, DRAFT, 1)))
                    sides[1].append(jnp.where(low, pltpu.roll(even, DRAFT, 1), odd_))
                at = pl.ds(pl.multiple_of(c * rows + (step - 2 * LAG) * QUAD * DRAFT, QUAD * DRAFT), QUAD * DRAFT)
                for side in range(2):
                    o_all[side, :, at, :] = jnp.concatenate(sides[side], axis=1).astype(jnp.bfloat16)

        mine = jnp.sum(jnp.where(low, acc, 0.0), axis=1)
        theirs = jnp.sum(jnp.where(low, 0.0, acc), axis=1)
        for slot in range(ring):
            s_all[0, c, slot] = mine[slot:slot + 1]
            s_all[1, c, slot] = theirs[slot:slot + 1]
        send(o_all.at[1, :, area], o_pair.at[:, area], po_send, po_recv.at[c], partner).start()
        send(s_all.at[1, c], s_pair.at[c], ps_send, ps_recv.at[c], partner).start()

    def weigh(stats):
        top = functools.reduce(jnp.maximum, stats)
        parts = [jnp.exp2(s - top) for s in stats]
        total = functools.reduce(jnp.add, parts)
        inv = 1.0 / total
        cols = [jnp.broadcast_to(p * inv, (LANES, LANES)).T for p in parts]
        return cols, top + jnp.log2(total)

    def mix(cols, blocks):
        return functools.reduce(jnp.add, [w * b.astype(jnp.float32) for w, b in zip(cols, blocks)])

    row_lane = lax.broadcasted_iota(jnp.int32, (1, LANES), 1)

    def reduce_hop(dist, c):
        area = chunk_rows(c)
        if dist == half:
            arrived(o_pair.at[:, area], po_recv.at[c])
            arrived(s_pair.at[c], ps_recv.at[c])
            cols, stat = weigh([s_all[0, c, half], s_pair[c, half]])
            o_all[0, half, area, :] = mix(cols, [o_all[0, half, area, :], o_pair[half, area, :]]).astype(jnp.bfloat16)
            s_all[0, c, half] = stat
            for way in range(2):
                send(o_all.at[0, half, split_rows(c, way)], o_half.at[way, half_rows_of(c)],
                     rs_send.at[way, half - 1], rs_recv.at[c, way, half - 1], beside[way]).start()
                send(s_all.at[0, c, half], s_in.at[way, half - 1, c],
                     ss_send.at[way, half - 1], ss_recv.at[c, way, half - 1], beside[way]).start()
            return
        for way in range(2):
            if dist == half - 1:
                arrived(o_half.at[way, half_rows_of(c)], rs_recv.at[c, way, dist])
            else:
                arrived(o_in.at[way, dist, area], rs_recv.at[c, way, dist])
            arrived(s_in.at[way, dist, c], ss_recv.at[c, way, dist])
            if dist == 0:
                continue
            slot = dist if way == 0 else ring - dist
            coming = s_in[way, dist, c]
            if dist == half - 1:
                coming = jnp.where((row_lane < half_rows) if way == 0 else (row_lane >= half_rows), coming, NEG_BIG)
            cols, stat = weigh([s_all[0, c, slot], s_pair[c, slot], coming])
            if dist == half - 1:
                for part in range(2):
                    at = split_rows(c, part)
                    blocks = [o_all[0, slot, at, :], o_pair[slot, at, :]]
                    if part == way:
                        blocks.append(o_half[way, half_rows_of(c), :])
                    cut = [w[part * half_rows:(part + 1) * half_rows] for w in cols]
                    o_all[0, slot, at, :] = mix(cut, blocks).astype(jnp.bfloat16)
            else:
                blocks = [o_all[0, slot, area, :], o_pair[slot, area, :], o_in[way, dist, area, :]]
                o_all[0, slot, area, :] = mix(cols, blocks).astype(jnp.bfloat16)
            s_all[0, c, slot] = stat
            send(o_all.at[0, slot, area], o_in.at[way, dist - 1, area],
                 rs_send.at[way, dist - 1], rs_recv.at[c, way, dist - 1], beside[way]).start()
            send(s_all.at[0, c, slot], s_in.at[way, dist - 1, c],
                 ss_send.at[way, dist - 1], ss_recv.at[c, way, dist - 1], beside[way]).start()
        if dist == 0:
            cols, _ = weigh([s_all[0, c, 0], s_pair[c, 0], s_in[0, 0, c], s_in[1, 0, c]])
            blocks = [o_all[0, 0, area, :], o_pair[0, area, :], o_in[0, 0, area, :], o_in[1, 0, area, :]]
            out_buf[area, :] = mix(cols, blocks).astype(jnp.bfloat16)
            pltpu.make_async_copy(out_buf.at[area], out_hbm.at[area], out_sem).start()

    stages = [(SKEW_GATHER[hop], functools.partial(gather, hop)) for hop in reversed(range(half + 1))]
    stages += [(SKEW_COMPUTE, compute)]
    stages += [(SKEW_REDUCE[dist], functools.partial(reduce_hop, dist)) for dist in range(half + 1)]

    @pl.loop(0, num_chunks + max(skew for skew, _ in stages))
    def _(step):
        for skew, stage in stages:
            c = step - skew

            @pl.when(jnp.logical_and(c >= 0, c < num_chunks))
            def _(stage=stage, c=c):
                stage(c)

    for way in range(2):
        for hop in range(half):
            area = pl.ds(0, num_chunks * (rows if hop + 1 < half else half_rows))
            arrived(q_all.at[0, hop, area], ag_send.at[way, hop])
            arrived(o_all.at[0, hop, area], rs_send.at[way, hop])
            arrived(s_in.at[way, hop], ss_send.at[way, hop])
    arrived(q_all.at[1], pq_send)
    arrived(o_all.at[1], po_send)
    arrived(s_all.at[1], ps_send)
    arrived(out_buf, out_sem)


def solution(mesh):
    dup_size = mesh.shape["dup"]
    ring = dup_size // 2
    half = ring // 2

    def group_step(q_local, k_span, v_span, len_local):
        num_batch, draft, head_dim = q_local.shape
        total_rows = num_batch * draft
        chunks = total_rows // LANES
        bf16, f32 = jnp.bfloat16, jnp.float32
        dma = pltpu.SemaphoreType.DMA
        out = pl.pallas_call(
            functools.partial(kernel, ring),
            out_shape=jax.ShapeDtypeStruct((total_rows, head_dim), bf16),
            in_specs=[pl.BlockSpec(memory_space=pltpu.SMEM)] + [pl.BlockSpec(memory_space=pl.ANY)] * 3,
            out_specs=pl.BlockSpec(memory_space=pl.ANY),
            scratch_shapes=[
                pltpu.VMEM((2, ring, total_rows, head_dim), bf16),
                pltpu.VMEM((2, ring, total_rows, head_dim), bf16),
                pltpu.VMEM((ring, total_rows, head_dim), bf16),
                pltpu.VMEM((2, half - 1, total_rows, head_dim), bf16),
                pltpu.VMEM((2, total_rows // 2, head_dim), bf16),
                pltpu.VMEM((2, chunks, ring, 1, LANES), f32),
                pltpu.VMEM((chunks, ring, 1, LANES), f32),
                pltpu.VMEM((2, half, chunks, 1, LANES), f32),
                pltpu.VMEM(k_span.shape, bf16),
                pltpu.VMEM(v_span.shape, bf16),
                pltpu.VMEM((total_rows, head_dim), bf16),
                dma, dma((chunks,)), dma((chunks,)), dma,
                dma((2, half)), dma((chunks, 2, half)), dma, dma((chunks,)),
                dma, dma((chunks,)), dma, dma((chunks,)),
                dma((2, half)), dma((chunks, 2, half)), dma((2, half)), dma((chunks, 2, half)),
            ],
            compiler_params=pltpu.CompilerParams(collective_id=0, has_side_effects=True, vmem_limit_bytes=60 * 1024 * 1024),
        )(len_local, q_local.reshape(total_rows, head_dim), k_span, v_span)
        return out.reshape(num_batch, draft, head_dim)

    return jax.shard_map(group_step, mesh=mesh, in_specs=(P("kv", "dup", None), P("kv", "dup", None), P("kv", "dup", None), P("kv")), out_specs=P("kv", "dup", None), check_vma=False)
```

```python
import functools
import math

import jax
import jax.numpy as jnp
from jax import lax
from jax.experimental import pallas as pl
from jax.experimental.pallas import tpu as pltpu
from jax.sharding import PartitionSpec as P

DRAFT = 4
NEG_BIG = -1e30
LANES = 128
QUAD = 4
LAG = 1
MESH_ID = pl.DeviceIdType.MESH

SKEW_GATHER = (0, 2, 4, 6, 8)
ORDER = [(0, 0, 5), (0, 0, 3), (0, 0, 7), (0, 0, 6), (0, 0, 2), (0, 1, 5), (0, 1, 3), (0, 1, 7), (0, 0, 4), (0, 0, 1), (0, 2, 5), (0, 0, 0), (0, 2, 3), (0, 1, 6), (0, 1, 4), (0, 3, 5), (0, 2, 7), (0, 1, 2), (0, 1, 1), (0, 2, 6), (0, 3, 3), (0, 4, 5), (0, 2, 4), (0, 3, 7), (0, 1, 0), (0, 2, 2), (1, 0, 5), (0, 3, 6), (0, 2, 1), (0, 4, 3), (2, 4, 5), (0, 4, 7), (0, 3, 4), (1, 0, 3), (0, 2, 0), (0, 3, 2), (0, 4, 6), (1, 0, 7), (0, 3, 1), (0, 4, 4), (2, 4, 3), (2, 3, 5), (1, 0, 6), (0, 3, 0), (2, 4, 7), (0, 4, 2), (1, 0, 4), (2, 4, 6), (2, 3, 3), (0, 4, 1), (1, 0, 2), (2, 3, 7), (2, 4, 4), (2, 2, 5), (0, 4, 0), (1, 0, 1), (2, 4, 2), (2, 2, 3), (2, 3, 6), (1, 0, 0), (2, 4, 1), (2, 3, 4), (2, 2, 7), (2, 4, 0), (2, 1, 5), (2, 3, 2), (2, 3, 1), (2, 2, 6), (2, 3, 0), (2, 2, 4), (2, 2, 2), (2, 2, 1), (2, 1, 3), (2, 2, 0), (2, 1, 4), (2, 1, 6), (2, 1, 1), (2, 0, 5), (2, 1, 2), (2, 1, 0), (2, 1, 7), (2, 0, 1), (2, 0, 6), (2, 0, 3), (2, 0, 4), (2, 0, 2), (2, 0, 0), (2, 0, 7)]
SKEW_REDUCE = (18, 16, 14, 12, 10)


def kernel(ring, len_ref, q_hbm, k_hbm, v_hbm, out_ref,
           q_all, o_all, o_pair, o_in, o_half, s_all, s_pair, s_in, k_buf, v_buf,
           q_sem, k_sem, v_sem, ag_send, ag_recv, pq_send, pq_recv,
           po_send, po_recv, ps_send, ps_recv, rs_send, rs_recv, ss_send, ss_recv):
    half = ring // 2
    num_chunks = s_all.shape[1]
    rows = LANES
    half_rows = rows // 2
    seqs = rows // DRAFT
    head_dim = q_hbm.shape[-1]
    span_len = k_hbm.shape[1]

    me = lax.axis_index("dup")
    z = me // 2
    core = lax.rem(me, 2)
    partner = me + 1 - 2 * core
    right = lax.rem(z + 1, ring) * 2 + core
    left = lax.rem(z + ring - 1, ring) * 2 + core
    beside = (right, left)

    def load_kv(c):
        span = pl.ds(c * seqs, seqs)
        return (pltpu.make_async_copy(k_hbm.at[span], k_buf.at[span], k_sem.at[c]),
                pltpu.make_async_copy(v_hbm.at[span], v_buf.at[span], v_sem.at[c]))

    load_q = pltpu.make_async_copy(q_hbm, q_all.at[0, 0], q_sem)
    load_q.start()

    barrier = pltpu.get_barrier_semaphore()
    for other in (right, left, partner):
        pl.semaphore_signal(barrier, inc=1, device_id={"dup": other}, device_id_type=MESH_ID)

    @pl.loop(0, num_chunks)
    def _(c):
        for copy in load_kv(c):
            copy.start()

    load_q.wait()
    pl.semaphore_wait(barrier, 3)

    def send(src, dst, send_sem, recv_sem, other):
        return pltpu.make_async_remote_copy(src_ref=src, dst_ref=dst, send_sem=send_sem, recv_sem=recv_sem,
                                            device_id={"dup": other}, device_id_type=MESH_ID)

    def arrived(ref, sem):
        pltpu.make_async_copy(ref, ref, sem).wait()

    def chunk_rows(c):
        return pl.ds(pl.multiple_of(c * rows, rows), rows)

    def split_rows(c, way):
        return pl.ds(pl.multiple_of(c * rows + way * half_rows, half_rows), half_rows)

    def half_rows_of(c):
        return pl.ds(pl.multiple_of(c * half_rows, half_rows), half_rows)

    def slot_at(way, hop):
        return lax.rem(ring - hop, ring) if way == 0 else hop

    def gather(hop, c):
        area = chunk_rows(c)
        slots = [(ring - hop) % ring, hop % ring]
        if 0 < hop < half:
            for way in range(2):
                arrived(q_all.at[0, slots[way], area], ag_recv.at[c, way, hop - 1])
        elif hop == half:
            for way in range(2):
                arrived(q_all.at[0, half, split_rows(c, way)], ag_recv.at[c, way, hop - 1])
        if hop < half:
            for way in range(2):
                part = area if hop + 1 < half else split_rows(c, way)
                to = (ring - hop - 1) if way == 0 else hop + 1
                send(q_all.at[0, slots[way], part], q_all.at[0, to, part],
                     ag_send.at[way, hop], ag_recv.at[c, way, hop], beside[way]).start()
        for slot in sorted(set(slots)):
            send(q_all.at[0, slot, area], q_all.at[1, slot, area], pq_send, pq_recv.at[c], partner).start()

    sub = lax.broadcasted_iota(jnp.int32, (8, LANES), 0)
    lane = lax.broadcasted_iota(jnp.int32, (8, LANES), 1)
    low = (sub < DRAFT)[None]
    lane_less_token = lane - lax.rem(sub, DRAFT)
    scale = math.log2(math.e) / math.sqrt(head_dim)

    def compute(c):
        area = chunk_rows(c)
        arrived(q_all.at[1, :, area], pq_recv.at[c])
        for copy in load_kv(c):
            copy.wait()
        acc = jnp.zeros((ring, 8, LANES), jnp.float32)
        quads = seqs // QUAD
        scores, probs = {}, {}
        for step in range(quads + 2 * LAG):
            if step < quads:
                r0 = pl.multiple_of(c * rows + step * QUAD * DRAFT, QUAD * DRAFT)
                q = q_all[:, :, pl.ds(r0, QUAD * DRAFT), :].astype(jnp.float32).reshape(2, ring, QUAD // 2, 8, head_dim)
                for pair in range(QUAD // 2):
                    mine, theirs = q[0, :, pair], q[1, :, pair]
                    both = (jnp.where(low, mine, pltpu.roll(theirs, DRAFT, 1)), jnp.where(low, pltpu.roll(mine, DRAFT, 1), theirs))
                    for odd in range(2):
                        local = step * QUAD + 2 * pair + odd
                        q_rows = both[odd].reshape(ring * 8, head_dim).astype(jnp.bfloat16)
                        scores[local] = lax.dot_general(q_rows, k_buf[c * seqs + local], (((1,), (1,)), ((), ())),
                                                        preferred_element_type=jnp.float32)
            if 0 <= step - LAG < quads:
                for local in range((step - LAG) * QUAD, (step - LAG + 1) * QUAD):
                    limit = len_ref[c * seqs + local] - DRAFT - me * span_len
                    s = scores.pop(local).reshape(ring, 8, span_len)
                    s = jnp.where((lane_less_token <= limit)[None], s, NEG_BIG)
                    peak = jnp.max(s, axis=2, keepdims=True)
                    p = jnp.exp2((s - peak) * scale)
                    mass = jnp.sum(p, axis=2, keepdims=True)
                    acc = jnp.where((lane_less_token == DRAFT * local)[None], peak * scale + jnp.log2(mass), acc)
                    probs[local] = (p.astype(jnp.bfloat16).reshape(ring * 8, span_len), 1.0 / mass)
            if 0 <= step - 2 * LAG < quads:
                outs = []
                for local in range((step - 2 * LAG) * QUAD, (step - 2 * LAG + 1) * QUAD):
                    p, inv = probs.pop(local)
                    o = jnp.dot(p, v_buf[c * seqs + local], preferred_element_type=jnp.float32)
                    outs.append(o.reshape(ring, 8, head_dim) * inv)
                sides = [[], []]
                for even, odd_ in zip(outs[0::2], outs[1::2]):
                    sides[0].append(jnp.where(low, even, pltpu.roll(odd_, DRAFT, 1)))
                    sides[1].append(jnp.where(low, pltpu.roll(even, DRAFT, 1), odd_))
                at = pl.ds(pl.multiple_of(c * rows + (step - 2 * LAG) * QUAD * DRAFT, QUAD * DRAFT), QUAD * DRAFT)
                for side in range(2):
                    o_all[side, :, at, :] = jnp.concatenate(sides[side], axis=1).astype(jnp.bfloat16)

        mine = jnp.sum(jnp.where(low, acc, 0.0), axis=1)
        theirs = jnp.sum(jnp.where(low, 0.0, acc), axis=1)
        for slot in range(ring):
            s_all[0, c, slot] = mine[slot:slot + 1]
            s_all[1, c, slot] = theirs[slot:slot + 1]
        send(o_all.at[1, :, area], o_pair.at[:, area], po_send, po_recv.at[c], partner).start()
        send(s_all.at[1, c], s_pair.at[c], ps_send, ps_recv.at[c], partner).start()

    def weigh(stats):
        top = functools.reduce(jnp.maximum, stats)
        parts = [jnp.exp2(s - top) for s in stats]
        total = functools.reduce(jnp.add, parts)
        inv = 1.0 / total
        cols = [jnp.broadcast_to(p * inv, (LANES, LANES)).T for p in parts]
        return cols, top + jnp.log2(total)

    def mix(cols, blocks):
        return functools.reduce(jnp.add, [w * b.astype(jnp.float32) for w, b in zip(cols, blocks)])

    row_lane = lax.broadcasted_iota(jnp.int32, (1, LANES), 1)

    def reduce_hop(dist, c):
        area = chunk_rows(c)
        if dist == half:
            arrived(o_pair.at[:, area], po_recv.at[c])
            arrived(s_pair.at[c], ps_recv.at[c])
            cols, stat = weigh([s_all[0, c, half], s_pair[c, half]])
            o_all[0, half, area, :] = mix(cols, [o_all[0, half, area, :], o_pair[half, area, :]]).astype(jnp.bfloat16)
            s_all[0, c, half] = stat
            for way in range(2):
                send(o_all.at[0, half, split_rows(c, way)], o_half.at[way, half_rows_of(c)],
                     rs_send.at[way, half - 1], rs_recv.at[c, way, half - 1], beside[way]).start()
                send(s_all.at[0, c, half], s_in.at[way, half - 1, c],
                     ss_send.at[way, half - 1], ss_recv.at[c, way, half - 1], beside[way]).start()
            return
        for way in range(2):
            if dist == half - 1:
                arrived(o_half.at[way, half_rows_of(c)], rs_recv.at[c, way, dist])
            else:
                arrived(o_in.at[way, dist, area], rs_recv.at[c, way, dist])
            arrived(s_in.at[way, dist, c], ss_recv.at[c, way, dist])
            if dist == 0:
                continue
            slot = dist if way == 0 else ring - dist
            coming = s_in[way, dist, c]
            if dist == half - 1:
                coming = jnp.where((row_lane < half_rows) if way == 0 else (row_lane >= half_rows), coming, NEG_BIG)
            cols, stat = weigh([s_all[0, c, slot], s_pair[c, slot], coming])
            if dist == half - 1:
                for part in range(2):
                    at = split_rows(c, part)
                    blocks = [o_all[0, slot, at, :], o_pair[slot, at, :]]
                    if part == way:
                        blocks.append(o_half[way, half_rows_of(c), :])
                    cut = [w[part * half_rows:(part + 1) * half_rows] for w in cols]
                    o_all[0, slot, at, :] = mix(cut, blocks).astype(jnp.bfloat16)
            else:
                blocks = [o_all[0, slot, area, :], o_pair[slot, area, :], o_in[way, dist, area, :]]
                o_all[0, slot, area, :] = mix(cols, blocks).astype(jnp.bfloat16)
            s_all[0, c, slot] = stat
            send(o_all.at[0, slot, area], o_in.at[way, dist - 1, area],
                 rs_send.at[way, dist - 1], rs_recv.at[c, way, dist - 1], beside[way]).start()
            send(s_all.at[0, c, slot], s_in.at[way, dist - 1, c],
                 ss_send.at[way, dist - 1], ss_recv.at[c, way, dist - 1], beside[way]).start()
        if dist == 0:
            cols, _ = weigh([s_all[0, c, 0], s_pair[c, 0], s_in[0, 0, c], s_in[1, 0, c]])
            blocks = [o_all[0, 0, area, :], o_pair[0, area, :], o_in[0, 0, area, :], o_in[1, 0, area, :]]
            out_ref[area, :] = mix(cols, blocks).astype(jnp.bfloat16)

    for kind, hop, c in ORDER:
        if kind == 0:
            gather(hop, c)
        elif kind == 1:
            compute(c)
        else:
            reduce_hop(hop, c)

    for way in range(2):
        for hop in range(half):
            area = pl.ds(0, num_chunks * (rows if hop + 1 < half else half_rows))
            arrived(q_all.at[0, hop, area], ag_send.at[way, hop])
            arrived(o_all.at[0, hop, area], rs_send.at[way, hop])
            arrived(s_in.at[way, hop], ss_send.at[way, hop])
    arrived(q_all.at[1], pq_send)
    arrived(o_all.at[1], po_send)
    arrived(s_all.at[1], ps_send)


def solution(mesh):
    dup_size = mesh.shape["dup"]
    ring = dup_size // 2
    half = ring // 2

    def group_step(q_local, k_span, v_span, len_local):
        num_batch, draft, head_dim = q_local.shape
        total_rows = num_batch * draft
        chunks = total_rows // LANES
        bf16, f32 = jnp.bfloat16, jnp.float32
        dma = pltpu.SemaphoreType.DMA
        out = pl.pallas_call(
            functools.partial(kernel, ring),
            out_shape=pltpu.VMEM((total_rows, head_dim), bf16),
            in_specs=[pl.BlockSpec(memory_space=pltpu.SMEM)] + [pl.BlockSpec(memory_space=pl.ANY)] * 3,
            out_specs=pl.BlockSpec(memory_space=pltpu.VMEM),
            scratch_shapes=[
                pltpu.VMEM((2, ring, total_rows, head_dim), bf16),
                pltpu.VMEM((2, ring, total_rows, head_dim), bf16),
                pltpu.VMEM((ring, total_rows, head_dim), bf16),
                pltpu.VMEM((2, half - 1, total_rows, head_dim), bf16),
                pltpu.VMEM((2, total_rows // 2, head_dim), bf16),
                pltpu.VMEM((2, chunks, ring, 1, LANES), f32),
                pltpu.VMEM((chunks, ring, 1, LANES), f32),
                pltpu.VMEM((2, half, chunks, 1, LANES), f32),
                pltpu.VMEM(k_span.shape, bf16),
                pltpu.VMEM(v_span.shape, bf16),
                dma, dma((chunks,)), dma((chunks,)),
                dma((2, half)), dma((chunks, 2, half)), dma, dma((chunks,)),
                dma, dma((chunks,)), dma, dma((chunks,)),
                dma((2, half)), dma((chunks, 2, half)), dma((2, half)), dma((chunks, 2, half)),
            ],
            compiler_params=pltpu.CompilerParams(collective_id=0, has_side_effects=True, vmem_limit_bytes=60 * 1024 * 1024),
        )(len_local, q_local.reshape(total_rows, head_dim), k_span, v_span)
        return out.reshape(num_batch, draft, head_dim)

    return jax.shard_map(group_step, mesh=mesh, in_specs=(P("kv", "dup", None), P("kv", "dup", None), P("kv", "dup", None), P("kv")), out_specs=P("kv", "dup", None), check_vma=False)
```

```python
import functools
import math

import jax
import jax.numpy as jnp
from jax import lax
from jax.experimental import pallas as pl
from jax.experimental.pallas import tpu as pltpu
from jax.sharding import PartitionSpec as P

DRAFT = 4
NEG_BIG = -1e30
LANES = 128
QUAD = 4
LAG = 1
MESH_ID = pl.DeviceIdType.MESH

SKEW_GATHER = (0, 2, 4, 6, 8)
ORDER = [(0, 0, 5), (0, 0, 3), (0, 0, 7), (0, 0, 6), (0, 0, 2), (0, 1, 5), (0, 1, 3), (0, 1, 7), (0, 0, 4), (0, 0, 1), (0, 2, 5), (0, 0, 0), (0, 2, 3), (0, 1, 6), (0, 1, 4), (0, 3, 5), (0, 2, 7), (0, 1, 2), (0, 1, 1), (0, 2, 6), (0, 3, 3), (0, 4, 5), (0, 2, 4), (0, 3, 7), (0, 1, 0), (0, 2, 2), (1, 0, 5), (0, 3, 6), (0, 2, 1), (0, 4, 3), (2, 4, 5), (0, 4, 7), (0, 3, 4), (1, 0, 3), (0, 2, 0), (0, 3, 2), (0, 4, 6), (1, 0, 7), (0, 3, 1), (0, 4, 4), (2, 4, 3), (2, 3, 5), (1, 0, 6), (0, 3, 0), (2, 4, 7), (0, 4, 2), (1, 0, 4), (2, 4, 6), (2, 3, 3), (0, 4, 1), (1, 0, 2), (2, 3, 7), (2, 4, 4), (2, 2, 5), (0, 4, 0), (1, 0, 1), (2, 4, 2), (2, 2, 3), (2, 3, 6), (1, 0, 0), (2, 4, 1), (2, 3, 4), (2, 2, 7), (2, 4, 0), (2, 1, 5), (2, 3, 2), (2, 3, 1), (2, 2, 6), (2, 3, 0), (2, 2, 4), (2, 2, 2), (2, 2, 1), (2, 1, 3), (2, 2, 0), (2, 1, 4), (2, 1, 6), (2, 1, 1), (2, 0, 5), (2, 1, 2), (2, 1, 0), (2, 1, 7), (2, 0, 1), (2, 0, 6), (2, 0, 3), (2, 0, 4), (2, 0, 2), (2, 0, 0), (2, 0, 7)]
SKEW_REDUCE = (18, 16, 14, 12, 10)


def kernel(ring, len_ref, q_hbm, k_hbm, v_hbm, out_ref,
           q_all, o_all, o_pair, o_in, o_half, s_all, s_pair, s_in, k_buf, v_buf,
           q_sem, k_sem, v_sem, ag_send, ag_recv, pq_send, pq_recv,
           po_send, po_recv, ps_send, ps_recv, rs_send, rs_recv, ss_send, ss_recv):
    half = ring // 2
    num_chunks = s_all.shape[1]
    rows = LANES
    half_rows = rows // 2
    seqs = rows // DRAFT
    head_dim = q_hbm.shape[-1]
    span_len = k_hbm.shape[1]

    me = lax.axis_index("dup")
    z = me // 2
    core = lax.rem(me, 2)
    partner = me + 1 - 2 * core
    right = lax.rem(z + 1, ring) * 2 + 1 - core
    left = lax.rem(z + ring - 1, ring) * 2 + 1 - core
    beside = (right, left)

    def load_kv(c):
        span = pl.ds(c * seqs, seqs)
        return (pltpu.make_async_copy(k_hbm.at[span], k_buf.at[span], k_sem.at[c]),
                pltpu.make_async_copy(v_hbm.at[span], v_buf.at[span], v_sem.at[c]))

    load_q = pltpu.make_async_copy(q_hbm, q_all.at[0, 0], q_sem)
    load_q.start()

    barrier = pltpu.get_barrier_semaphore()
    for other in (right, left, partner):
        pl.semaphore_signal(barrier, inc=1, device_id={"dup": other}, device_id_type=MESH_ID)

    @pl.loop(0, num_chunks)
    def _(c):
        for copy in load_kv(c):
            copy.start()

    load_q.wait()
    pl.semaphore_wait(barrier, 3)

    def send(src, dst, send_sem, recv_sem, other):
        return pltpu.make_async_remote_copy(src_ref=src, dst_ref=dst, send_sem=send_sem, recv_sem=recv_sem,
                                            device_id={"dup": other}, device_id_type=MESH_ID)

    def arrived(ref, sem):
        pltpu.make_async_copy(ref, ref, sem).wait()

    def chunk_rows(c):
        return pl.ds(pl.multiple_of(c * rows, rows), rows)

    def split_rows(c, way):
        return pl.ds(pl.multiple_of(c * rows + way * half_rows, half_rows), half_rows)

    def half_rows_of(c):
        return pl.ds(pl.multiple_of(c * half_rows, half_rows), half_rows)

    def slot_at(way, hop):
        return lax.rem(ring - hop, ring) if way == 0 else hop

    def gather(hop, c):
        area = chunk_rows(c)
        slots = [(ring - hop) % ring, hop % ring]
        if 0 < hop < half:
            for way in range(2):
                arrived(q_all.at[0, slots[way], area], ag_recv.at[c, way, hop - 1])
        elif hop == half:
            for way in range(2):
                arrived(q_all.at[0, half, split_rows(c, way)], ag_recv.at[c, way, hop - 1])
        if hop < half:
            for way in range(2):
                part = area if hop + 1 < half else split_rows(c, way)
                to = (ring - hop - 1) if way == 0 else hop + 1
                send(q_all.at[0, slots[way], part], q_all.at[0, to, part],
                     ag_send.at[way, hop], ag_recv.at[c, way, hop], beside[way]).start()
        for slot in sorted(set(slots)):
            send(q_all.at[0, slot, area], q_all.at[1, slot, area], pq_send, pq_recv.at[c], partner).start()

    sub = lax.broadcasted_iota(jnp.int32, (8, LANES), 0)
    lane = lax.broadcasted_iota(jnp.int32, (8, LANES), 1)
    low = (sub < DRAFT)[None]
    lane_less_token = lane - lax.rem(sub, DRAFT)
    scale = math.log2(math.e) / math.sqrt(head_dim)

    def compute(c):
        area = chunk_rows(c)
        arrived(q_all.at[1, :, area], pq_recv.at[c])
        for copy in load_kv(c):
            copy.wait()
        acc = jnp.zeros((ring, 8, LANES), jnp.float32)
        quads = seqs // QUAD
        scores, probs = {}, {}
        for step in range(quads + 2 * LAG):
            if step < quads:
                r0 = pl.multiple_of(c * rows + step * QUAD * DRAFT, QUAD * DRAFT)
                q = q_all[:, :, pl.ds(r0, QUAD * DRAFT), :].astype(jnp.float32).reshape(2, ring, QUAD // 2, 8, head_dim)
                for pair in range(QUAD // 2):
                    mine, theirs = q[0, :, pair], q[1, :, pair]
                    both = (jnp.where(low, mine, pltpu.roll(theirs, DRAFT, 1)), jnp.where(low, pltpu.roll(mine, DRAFT, 1), theirs))
                    for odd in range(2):
                        local = step * QUAD + 2 * pair + odd
                        q_rows = both[odd].reshape(ring * 8, head_dim).astype(jnp.bfloat16)
                        scores[local] = lax.dot_general(q_rows, k_buf[c * seqs + local], (((1,), (1,)), ((), ())),
                                                        preferred_element_type=jnp.float32)
            if 0 <= step - LAG < quads:
                for local in range((step - LAG) * QUAD, (step - LAG + 1) * QUAD):
                    limit = len_ref[c * seqs + local] - DRAFT - me * span_len
                    s = scores.pop(local).reshape(ring, 8, span_len)
                    s = jnp.where((lane_less_token <= limit)[None], s, NEG_BIG)
                    peak = jnp.max(s, axis=2, keepdims=True)
                    p = jnp.exp2((s - peak) * scale)
                    mass = jnp.sum(p, axis=2, keepdims=True)
                    acc = jnp.where((lane_less_token == DRAFT * local)[None], peak * scale + jnp.log2(mass), acc)
                    probs[local] = (p.astype(jnp.bfloat16).reshape(ring * 8, span_len), 1.0 / mass)
            if 0 <= step - 2 * LAG < quads:
                outs = []
                for local in range((step - 2 * LAG) * QUAD, (step - 2 * LAG + 1) * QUAD):
                    p, inv = probs.pop(local)
                    o = jnp.dot(p, v_buf[c * seqs + local], preferred_element_type=jnp.float32)
                    outs.append(o.reshape(ring, 8, head_dim) * inv)
                sides = [[], []]
                for even, odd_ in zip(outs[0::2], outs[1::2]):
                    sides[0].append(jnp.where(low, even, pltpu.roll(odd_, DRAFT, 1)))
                    sides[1].append(jnp.where(low, pltpu.roll(even, DRAFT, 1), odd_))
                at = pl.ds(pl.multiple_of(c * rows + (step - 2 * LAG) * QUAD * DRAFT, QUAD * DRAFT), QUAD * DRAFT)
                for side in range(2):
                    o_all[side, :, at, :] = jnp.concatenate(sides[side], axis=1).astype(jnp.bfloat16)

        mine = jnp.sum(jnp.where(low, acc, 0.0), axis=1)
        theirs = jnp.sum(jnp.where(low, 0.0, acc), axis=1)
        for slot in range(ring):
            s_all[0, c, slot] = mine[slot:slot + 1]
            s_all[1, c, slot] = theirs[slot:slot + 1]
        send(o_all.at[1, :, area], o_pair.at[:, area], po_send, po_recv.at[c], partner).start()
        send(s_all.at[1, c], s_pair.at[c], ps_send, ps_recv.at[c], partner).start()

    def weigh(stats):
        top = functools.reduce(jnp.maximum, stats)
        parts = [jnp.exp2(s - top) for s in stats]
        total = functools.reduce(jnp.add, parts)
        inv = 1.0 / total
        cols = [jnp.broadcast_to(p * inv, (LANES, LANES)).T for p in parts]
        return cols, top + jnp.log2(total)

    def mix(cols, blocks):
        return functools.reduce(jnp.add, [w * b.astype(jnp.float32) for w, b in zip(cols, blocks)])

    row_lane = lax.broadcasted_iota(jnp.int32, (1, LANES), 1)

    def reduce_hop(dist, c):
        area = chunk_rows(c)
        if dist == half:
            arrived(o_pair.at[:, area], po_recv.at[c])
            arrived(s_pair.at[c], ps_recv.at[c])
            cols, stat = weigh([s_all[0, c, half], s_pair[c, half]])
            o_all[0, half, area, :] = mix(cols, [o_all[0, half, area, :], o_pair[half, area, :]]).astype(jnp.bfloat16)
            s_all[0, c, half] = stat
            for way in range(2):
                send(o_all.at[0, half, split_rows(c, way)], o_half.at[way, half_rows_of(c)],
                     rs_send.at[way, half - 1], rs_recv.at[c, way, half - 1], beside[way]).start()
                send(s_all.at[0, c, half], s_in.at[way, half - 1, c],
                     ss_send.at[way, half - 1], ss_recv.at[c, way, half - 1], beside[way]).start()
            return
        for way in range(2):
            if dist == half - 1:
                arrived(o_half.at[way, half_rows_of(c)], rs_recv.at[c, way, dist])
            else:
                arrived(o_in.at[way, dist, area], rs_recv.at[c, way, dist])
            arrived(s_in.at[way, dist, c], ss_recv.at[c, way, dist])
        slots = (dist, ring - dist) if dist else ()
        weights = []
        for way, slot in enumerate(slots):
            coming = s_in[way, dist, c]
            if dist == half - 1:
                coming = jnp.where((row_lane < half_rows) if way == 0 else (row_lane >= half_rows), coming, NEG_BIG)
            weights.append(weigh([s_all[0, c, slot], s_pair[c, slot], coming]))
        for way, slot in enumerate(slots):
            cols, stat = weights[way]
            s_all[0, c, slot] = stat
            if dist == half - 1:
                for part in range(2):
                    at = split_rows(c, part)
                    blocks = [o_all[0, slot, at, :], o_pair[slot, at, :]]
                    if part == way:
                        blocks.append(o_half[way, half_rows_of(c), :])
                    cut = [w[part * half_rows:(part + 1) * half_rows] for w in cols]
                    o_all[0, slot, at, :] = mix(cut, blocks).astype(jnp.bfloat16)
            else:
                blocks = [o_all[0, slot, area, :], o_pair[slot, area, :], o_in[way, dist, area, :]]
                o_all[0, slot, area, :] = mix(cols, blocks).astype(jnp.bfloat16)
            send(o_all.at[0, slot, area], o_in.at[way, dist - 1, area],
                 rs_send.at[way, dist - 1], rs_recv.at[c, way, dist - 1], beside[way]).start()
            send(s_all.at[0, c, slot], s_in.at[way, dist - 1, c],
                 ss_send.at[way, dist - 1], ss_recv.at[c, way, dist - 1], beside[way]).start()
        if dist == 0:
            cols, _ = weigh([s_all[0, c, 0], s_pair[c, 0], s_in[0, 0, c], s_in[1, 0, c]])
            blocks = [o_all[0, 0, area, :], o_pair[0, area, :], o_in[0, 0, area, :], o_in[1, 0, area, :]]
            out_ref[area, :] = mix(cols, blocks).astype(jnp.bfloat16)

    for kind, hop, c in ORDER:
        if kind == 0:
            gather(hop, c)
        elif kind == 1:
            compute(c)
        else:
            reduce_hop(hop, c)

    for way in range(2):
        for hop in range(half):
            area = pl.ds(0, num_chunks * (rows if hop + 1 < half else half_rows))
            arrived(q_all.at[0, hop, area], ag_send.at[way, hop])
            arrived(o_all.at[0, hop, area], rs_send.at[way, hop])
            arrived(s_in.at[way, hop], ss_send.at[way, hop])
    arrived(q_all.at[1], pq_send)
    arrived(o_all.at[1], po_send)
    arrived(s_all.at[1], ps_send)


def solution(mesh):
    dup_size = mesh.shape["dup"]
    ring = dup_size // 2
    half = ring // 2

    def group_step(q_local, k_span, v_span, len_local):
        num_batch, draft, head_dim = q_local.shape
        total_rows = num_batch * draft
        chunks = total_rows // LANES
        bf16, f32 = jnp.bfloat16, jnp.float32
        dma = pltpu.SemaphoreType.DMA
        out = pl.pallas_call(
            functools.partial(kernel, ring),
            out_shape=pltpu.VMEM((total_rows, head_dim), bf16),
            in_specs=[pl.BlockSpec(memory_space=pltpu.SMEM)] + [pl.BlockSpec(memory_space=pl.ANY)] * 3,
            out_specs=pl.BlockSpec(memory_space=pltpu.VMEM),
            scratch_shapes=[
                pltpu.VMEM((2, ring, total_rows, head_dim), bf16),
                pltpu.VMEM((2, ring, total_rows, head_dim), bf16),
                pltpu.VMEM((ring, total_rows, head_dim), bf16),
                pltpu.VMEM((2, half - 1, total_rows, head_dim), bf16),
                pltpu.VMEM((2, total_rows // 2, head_dim), bf16),
                pltpu.VMEM((2, chunks, ring, 1, LANES), f32),
                pltpu.VMEM((chunks, ring, 1, LANES), f32),
                pltpu.VMEM((2, half, chunks, 1, LANES), f32),
                pltpu.VMEM(k_span.shape, bf16),
                pltpu.VMEM(v_span.shape, bf16),
                dma, dma((chunks,)), dma((chunks,)),
                dma((2, half)), dma((chunks, 2, half)), dma, dma((chunks,)),
                dma, dma((chunks,)), dma, dma((chunks,)),
                dma((2, half)), dma((chunks, 2, half)), dma((2, half)), dma((chunks, 2, half)),
            ],
            compiler_params=pltpu.CompilerParams(collective_id=0, has_side_effects=True, vmem_limit_bytes=60 * 1024 * 1024),
        )(len_local, q_local.reshape(total_rows, head_dim), k_span, v_span)
        return out.reshape(num_batch, draft, head_dim)

    return jax.shard_map(group_step, mesh=mesh, in_specs=(P("kv", "dup", None), P("kv", "dup", None), P("kv", "dup", None), P("kv")), out_specs=P("kv", "dup", None), check_vma=False)
```

```python
import functools
import math

import jax
import jax.numpy as jnp
from jax import lax
from jax.experimental import pallas as pl
from jax.experimental.pallas import tpu as pltpu
from jax.sharding import PartitionSpec as P

DRAFT = 4
NEG_BIG = -1e30
LANES = 128
QUAD = 4
LAG = 1
MESH_ID = pl.DeviceIdType.MESH

SKEW_GATHER = (0, 2, 4, 6, 8)
ORDER = [(0, 0, 5), (0, 0, 3), (0, 0, 7), (0, 0, 6), (0, 0, 2), (0, 1, 5), (0, 1, 3), (0, 1, 7), (0, 0, 4), (0, 0, 1), (0, 2, 5), (0, 0, 0), (0, 2, 3), (0, 1, 6), (0, 1, 4), (0, 3, 5), (0, 2, 7), (0, 1, 2), (0, 1, 1), (0, 2, 6), (0, 3, 3), (0, 4, 5), (0, 2, 4), (0, 3, 7), (0, 1, 0), (0, 2, 2), (1, 0, 5), (0, 3, 6), (0, 2, 1), (0, 4, 3), (2, 4, 5), (0, 4, 7), (0, 3, 4), (1, 0, 3), (0, 2, 0), (0, 3, 2), (0, 4, 6), (1, 0, 7), (0, 3, 1), (0, 4, 4), (2, 4, 3), (2, 3, 5), (1, 0, 6), (0, 3, 0), (2, 4, 7), (0, 4, 2), (1, 0, 4), (2, 4, 6), (2, 3, 3), (0, 4, 1), (1, 0, 2), (2, 3, 7), (2, 4, 4), (2, 2, 5), (0, 4, 0), (1, 0, 1), (2, 4, 2), (2, 2, 3), (2, 3, 6), (1, 0, 0), (2, 4, 1), (2, 3, 4), (2, 2, 7), (2, 4, 0), (2, 1, 5), (2, 3, 2), (2, 3, 1), (2, 2, 6), (2, 3, 0), (2, 2, 4), (2, 2, 2), (2, 2, 1), (2, 1, 3), (2, 2, 0), (2, 1, 4), (2, 1, 6), (2, 1, 1), (2, 0, 5), (2, 1, 2), (2, 1, 0), (2, 1, 7), (2, 0, 1), (2, 0, 6), (2, 0, 3), (2, 0, 4), (2, 0, 2), (2, 0, 0), (2, 0, 7)]
SKEW_REDUCE = (18, 16, 14, 12, 10)


def kernel(ring, len_ref, q_hbm, k_hbm, v_hbm, out_ref,
           q_all, o_all, o_pair, o_in, o_half, s_all, s_pair, s_in, k_buf, v_buf,
           q_sem, k_sem, v_sem, ag_send, ag_recv, pq_send, pq_recv,
           po_send, po_recv, ps_send, ps_recv, rs_send, rs_recv, ss_send, ss_recv):
    half = ring // 2
    num_chunks = s_all.shape[1]
    rows = LANES
    half_rows = rows // 2
    seqs = rows // DRAFT
    head_dim = q_hbm.shape[-1]
    span_len = k_hbm.shape[1]

    me = lax.axis_index("dup")
    z = me // 2
    core = lax.rem(me, 2)
    partner = me + 1 - 2 * core
    right = lax.rem(z + 1, ring) * 2 + 1 - core
    left = lax.rem(z + ring - 1, ring) * 2 + 1 - core
    beside = (right, left)

    def load_kv(c):
        span = pl.ds(c * seqs, seqs)
        return (pltpu.make_async_copy(k_hbm.at[span], k_buf.at[span], k_sem.at[c]),
                pltpu.make_async_copy(v_hbm.at[span], v_buf.at[span], v_sem.at[c]))

    load_q = pltpu.make_async_copy(q_hbm, q_all.at[0, 0], q_sem)
    load_q.start()

    barrier = pltpu.get_barrier_semaphore()
    for other in (right, left, partner):
        pl.semaphore_signal(barrier, inc=1, device_id={"dup": other}, device_id_type=MESH_ID)

    @pl.loop(0, num_chunks)
    def _(c):
        for copy in load_kv(c):
            copy.start()

    load_q.wait()
    pl.semaphore_wait(barrier, 3)

    def send(src, dst, send_sem, recv_sem, other):
        return pltpu.make_async_remote_copy(src_ref=src, dst_ref=dst, send_sem=send_sem, recv_sem=recv_sem,
                                            device_id={"dup": other}, device_id_type=MESH_ID)

    def arrived(ref, sem):
        pltpu.make_async_copy(ref, ref, sem).wait()

    def chunk_rows(c):
        return pl.ds(pl.multiple_of(c * rows, rows), rows)

    def split_rows(c, way):
        return pl.ds(pl.multiple_of(c * rows + way * half_rows, half_rows), half_rows)

    def half_rows_of(c):
        return pl.ds(pl.multiple_of(c * half_rows, half_rows), half_rows)

    def slot_of(way, dist):
        return 0 if dist == 0 else ring - 1 if dist == half else 2 * dist - 1 + way

    def gather(hop, c):
        area = chunk_rows(c)
        slots = [slot_of(1 - way, hop) for way in range(2)]
        if 0 < hop < half:
            for way in range(2):
                arrived(q_all.at[0, slots[way], area], ag_recv.at[c, way, hop - 1])
        elif hop == half:
            for way in range(2):
                arrived(q_all.at[0, ring - 1, split_rows(c, way)], ag_recv.at[c, way, hop - 1])
        if hop < half:
            for way in range(2):
                part = area if hop + 1 < half else split_rows(c, way)
                to = slot_of(1 - way, hop + 1)
                send(q_all.at[0, slots[way], part], q_all.at[0, to, part],
                     ag_send.at[way, hop], ag_recv.at[c, way, hop], beside[way]).start()
        both = pl.ds(min(slots), len(set(slots)))
        send(q_all.at[0, both, area], q_all.at[1, both, area], pq_send, pq_recv.at[c], partner).start()

    sub = lax.broadcasted_iota(jnp.int32, (8, LANES), 0)
    lane = lax.broadcasted_iota(jnp.int32, (8, LANES), 1)
    low = (sub < DRAFT)[None]
    lane_less_token = lane - lax.rem(sub, DRAFT)
    scale = math.log2(math.e) / math.sqrt(head_dim)

    def compute(c):
        area = chunk_rows(c)
        arrived(q_all.at[1, :, area], pq_recv.at[c])
        for copy in load_kv(c):
            copy.wait()
        acc = jnp.zeros((ring, 8, LANES), jnp.float32)
        quads = seqs // QUAD
        scores, probs = {}, {}
        for step in range(quads + 2 * LAG):
            if step < quads:
                r0 = pl.multiple_of(c * rows + step * QUAD * DRAFT, QUAD * DRAFT)
                q = q_all[:, :, pl.ds(r0, QUAD * DRAFT), :].astype(jnp.float32).reshape(2, ring, QUAD // 2, 8, head_dim)
                for pair in range(QUAD // 2):
                    mine, theirs = q[0, :, pair], q[1, :, pair]
                    both = (jnp.where(low, mine, pltpu.roll(theirs, DRAFT, 1)), jnp.where(low, pltpu.roll(mine, DRAFT, 1), theirs))
                    for odd in range(2):
                        local = step * QUAD + 2 * pair + odd
                        q_rows = both[odd].reshape(ring * 8, head_dim).astype(jnp.bfloat16)
                        scores[local] = lax.dot_general(q_rows, k_buf[c * seqs + local], (((1,), (1,)), ((), ())),
                                                        preferred_element_type=jnp.float32)
            if 0 <= step - LAG < quads:
                for local in range((step - LAG) * QUAD, (step - LAG + 1) * QUAD):
                    limit = len_ref[c * seqs + local] - DRAFT - me * span_len
                    s = scores.pop(local).reshape(ring, 8, span_len)
                    s = jnp.where((lane_less_token <= limit)[None], s, NEG_BIG)
                    peak = jnp.max(s, axis=2, keepdims=True)
                    p = jnp.exp2((s - peak) * scale)
                    mass = jnp.sum(p, axis=2, keepdims=True)
                    acc = jnp.where((lane_less_token == DRAFT * local)[None], peak * scale + jnp.log2(mass), acc)
                    probs[local] = (p.astype(jnp.bfloat16).reshape(ring * 8, span_len), 1.0 / mass)
            if 0 <= step - 2 * LAG < quads:
                outs = []
                for local in range((step - 2 * LAG) * QUAD, (step - 2 * LAG + 1) * QUAD):
                    p, inv = probs.pop(local)
                    o = jnp.dot(p, v_buf[c * seqs + local], preferred_element_type=jnp.float32)
                    outs.append(o.reshape(ring, 8, head_dim) * inv)
                sides = [[], []]
                for even, odd_ in zip(outs[0::2], outs[1::2]):
                    sides[0].append(jnp.where(low, even, pltpu.roll(odd_, DRAFT, 1)))
                    sides[1].append(jnp.where(low, pltpu.roll(even, DRAFT, 1), odd_))
                at = pl.ds(pl.multiple_of(c * rows + (step - 2 * LAG) * QUAD * DRAFT, QUAD * DRAFT), QUAD * DRAFT)
                for side in range(2):
                    o_all[side, :, at, :] = jnp.concatenate(sides[side], axis=1).astype(jnp.bfloat16)

        mine = jnp.sum(jnp.where(low, acc, 0.0), axis=1)
        theirs = jnp.sum(jnp.where(low, 0.0, acc), axis=1)
        for slot in range(ring):
            s_all[0, c, slot] = mine[slot:slot + 1]
            s_all[1, c, slot] = theirs[slot:slot + 1]
        send(o_all.at[1, :, area], o_pair.at[:, area], po_send, po_recv.at[c], partner).start()
        send(s_all.at[1, c], s_pair.at[c], ps_send, ps_recv.at[c], partner).start()

    def weigh(stats):
        top = functools.reduce(jnp.maximum, stats)
        parts = [jnp.exp2(s - top) for s in stats]
        total = functools.reduce(jnp.add, parts)
        inv = 1.0 / total
        cols = [jnp.broadcast_to(p * inv, (LANES, LANES)).T for p in parts]
        return cols, top + jnp.log2(total)

    def mix(cols, blocks):
        return functools.reduce(jnp.add, [w * b.astype(jnp.float32) for w, b in zip(cols, blocks)])

    row_lane = lax.broadcasted_iota(jnp.int32, (1, LANES), 1)

    def reduce_hop(dist, c):
        area = chunk_rows(c)
        if dist == half:
            arrived(o_pair.at[:, area], po_recv.at[c])
            arrived(s_pair.at[c], ps_recv.at[c])
            cols, stat = weigh([s_all[0, c, ring - 1], s_pair[c, ring - 1]])
            o_all[0, ring - 1, area, :] = mix(cols, [o_all[0, ring - 1, area, :], o_pair[ring - 1, area, :]]).astype(jnp.bfloat16)
            s_all[0, c, ring - 1] = stat
            for way in range(2):
                send(o_all.at[0, ring - 1, split_rows(c, way)], o_half.at[way, half_rows_of(c)],
                     rs_send.at[way, half - 1], rs_recv.at[c, way, half - 1], beside[way]).start()
                send(s_all.at[0, c, ring - 1], s_in.at[way, half - 1, c],
                     ss_send.at[way, half - 1], ss_recv.at[c, way, half - 1], beside[way]).start()
            return
        for way in range(2):
            if dist == half - 1:
                arrived(o_half.at[way, half_rows_of(c)], rs_recv.at[c, way, dist])
            else:
                arrived(o_in.at[way, dist, area], rs_recv.at[c, way, dist])
            arrived(s_in.at[way, dist, c], ss_recv.at[c, way, dist])
        slots = (slot_of(0, dist), slot_of(1, dist)) if dist else ()
        weights = []
        for way, slot in enumerate(slots):
            coming = s_in[way, dist, c]
            if dist == half - 1:
                coming = jnp.where((row_lane < half_rows) if way == 0 else (row_lane >= half_rows), coming, NEG_BIG)
            weights.append(weigh([s_all[0, c, slot], s_pair[c, slot], coming]))
        for way, slot in enumerate(slots):
            cols, stat = weights[way]
            s_all[0, c, slot] = stat
            if dist == half - 1:
                for part in range(2):
                    at = split_rows(c, part)
                    blocks = [o_all[0, slot, at, :], o_pair[slot, at, :]]
                    if part == way:
                        blocks.append(o_half[way, half_rows_of(c), :])
                    cut = [w[part * half_rows:(part + 1) * half_rows] for w in cols]
                    o_all[0, slot, at, :] = mix(cut, blocks).astype(jnp.bfloat16)
            else:
                blocks = [o_all[0, slot, area, :], o_pair[slot, area, :], o_in[way, dist, area, :]]
                o_all[0, slot, area, :] = mix(cols, blocks).astype(jnp.bfloat16)
            send(o_all.at[0, slot, area], o_in.at[way, dist - 1, area],
                 rs_send.at[way, dist - 1], rs_recv.at[c, way, dist - 1], beside[way]).start()
            send(s_all.at[0, c, slot], s_in.at[way, dist - 1, c],
                 ss_send.at[way, dist - 1], ss_recv.at[c, way, dist - 1], beside[way]).start()
        if dist == 0:
            cols, _ = weigh([s_all[0, c, 0], s_pair[c, 0], s_in[0, 0, c], s_in[1, 0, c]])
            blocks = [o_all[0, 0, area, :], o_pair[0, area, :], o_in[0, 0, area, :], o_in[1, 0, area, :]]
            out_ref[area, :] = mix(cols, blocks).astype(jnp.bfloat16)

    def sends_done():
        for way in range(2):
            for hop in range(half):
                area = pl.ds(0, num_chunks * (rows if hop + 1 < half else half_rows))
                arrived(q_all.at[0, hop, area], ag_send.at[way, hop])
                arrived(o_all.at[0, hop, area], rs_send.at[way, hop])
                arrived(s_in.at[way, hop], ss_send.at[way, hop])
        arrived(q_all.at[1], pq_send)
        arrived(o_all.at[1], po_send)
        arrived(s_all.at[1], ps_send)

    for at, (kind, hop, c) in enumerate(ORDER):
        if at == len(ORDER) - 1:
            sends_done()
        if kind == 0:
            gather(hop, c)
        elif kind == 1:
            compute(c)
        else:
            reduce_hop(hop, c)


def solution(mesh):
    dup_size = mesh.shape["dup"]
    ring = dup_size // 2
    half = ring // 2

    def group_step(q_local, k_span, v_span, len_local):
        num_batch, draft, head_dim = q_local.shape
        total_rows = num_batch * draft
        chunks = total_rows // LANES
        bf16, f32 = jnp.bfloat16, jnp.float32
        dma = pltpu.SemaphoreType.DMA
        out = pl.pallas_call(
            functools.partial(kernel, ring),
            out_shape=pltpu.VMEM((total_rows, head_dim), bf16),
            in_specs=[pl.BlockSpec(memory_space=pltpu.SMEM)] + [pl.BlockSpec(memory_space=pl.ANY)] * 3,
            out_specs=pl.BlockSpec(memory_space=pltpu.VMEM),
            scratch_shapes=[
                pltpu.VMEM((2, ring, total_rows, head_dim), bf16),
                pltpu.VMEM((2, ring, total_rows, head_dim), bf16),
                pltpu.VMEM((ring, total_rows, head_dim), bf16),
                pltpu.VMEM((2, half - 1, total_rows, head_dim), bf16),
                pltpu.VMEM((2, total_rows // 2, head_dim), bf16),
                pltpu.VMEM((2, chunks, ring, 1, LANES), f32),
                pltpu.VMEM((chunks, ring, 1, LANES), f32),
                pltpu.VMEM((2, half, chunks, 1, LANES), f32),
                pltpu.VMEM(k_span.shape, bf16),
                pltpu.VMEM(v_span.shape, bf16),
                dma, dma((chunks,)), dma((chunks,)),
                dma((2, half)), dma((chunks, 2, half)), dma, dma((chunks,)),
                dma, dma((chunks,)), dma, dma((chunks,)),
                dma((2, half)), dma((chunks, 2, half)), dma((2, half)), dma((chunks, 2, half)),
            ],
            compiler_params=pltpu.CompilerParams(collective_id=0, has_side_effects=True, vmem_limit_bytes=60 * 1024 * 1024),
        )(len_local, q_local.reshape(total_rows, head_dim), k_span, v_span)
        return out.reshape(num_batch, draft, head_dim)

    return jax.shard_map(group_step, mesh=mesh, in_specs=(P("kv", "dup", None), P("kv", "dup", None), P("kv", "dup", None), P("kv")), out_specs=P("kv", "dup", None), check_vma=False)
```
